32 devices in a mesh: head: 4 (over x, core), ctx: 8 (over z, y).
Axes of the slice: x: 2, y: 2, z: 4, core: 2. Of those that a mesh axis runs over, the one named last changes fastest.
Arguments:
- query: bfloat16 [2048, 16384], P(('head', 'ctx')), may hold values from -5 to 5
- key: bfloat16 [2048, 1024], P(('head', 'ctx')), may hold values from -5 to 5
- value: bfloat16 [2048, 1024], P(('head', 'ctx')), may hold values from -6 to 6
- block_order: int32 [32], replicated, may hold values from 0 to 31, each once
Outputs:
- attended: bfloat16 [2048, 16384], P(('head', 'ctx'))
- log_norm_rows: float32 [2048, 128], P(('head', 'ctx'))
The draws below stay inside these ranges and needn't reach their ends.
All inputs are finite; a program needn't handle non-finite values.
Results may differ from the reference program's by a relative error of at most 0.0036.
Values may be sent and summed in bfloat16 or wider, within the bound.
No kernel may reach another device: no remote copies, remote signals or barrier semaphores. Data moves between devices by JAX's collectives and lax.ppermute only.
A program may use at most 64 MiB of HBM per device.

```python
import math
import jax
import jax.numpy as jnp
from jax import lax

HQ = 128
KEY_VALUE_HEADS = 8
HEAD_DIMENSION = 128
BLOCK_ROWS = 64
SEQUENCE_TOKENS = 2048
N_HEAD = 4
N_CTX = 8


def draw_common(key, salt, width):
    fresh = jax.random.fold_in(key, salt)
    base = jnp.clip(jax.random.normal(fresh, (SEQUENCE_TOKENS, width), jnp.float32), -4.5, 4.5)
    return base


def draw_query(key, part):
    return draw_common(key, 3, HQ * HEAD_DIMENSION).astype(jnp.bfloat16)


def draw_key(key, part):
    return draw_common(key, 5, KEY_VALUE_HEADS * HEAD_DIMENSION).astype(jnp.bfloat16)


def shard_levels(own_key, dims, pieces, low, top_value):
    factor_of, own = 1.0, jax.random.fold_in(own_key, 6)
    for position, blocks in pieces:
        heights = jnp.exp(jax.random.uniform(jax.random.fold_in(own, position), (blocks,), jnp.float32, low / len(pieces), top_value / len(pieces)))
        factor_of = factor_of * jnp.repeat(heights, dims[position] // blocks).reshape([-1 if axis == position else 1 for axis in range(len(dims))])
    return factor_of


def noise(key, dims, scale, limit, shards=(), kind=jnp.bfloat16):
    values = jax.random.normal(key, dims, jnp.float32) * scale
    if len(shards) > 0:
        values = shard_levels(key, dims, shards, -0.22, 0.18) * values
    return jnp.clip(values, min=-limit, max=limit).astype(kind)


def setup_inputs(seed: int = 0) -> dict:
    key_list = jax.random.split(jax.random.key(seed), 5)
    return {
        "query": draw_query(jax.random.fold_in(key_list[4], 71), 0),
        "key": draw_key(jax.random.fold_in(key_list[4], 71), 0),
        "value": noise(key_list[2], (SEQUENCE_TOKENS, KEY_VALUE_HEADS * HEAD_DIMENSION), 1.0, 6.0, ((0, 32),)),
        "block_order": jax.random.permutation(key_list[3], SEQUENCE_TOKENS // BLOCK_ROWS).astype(jnp.int32),
    }


def shard_rows(array, shard):
    blocks = array.reshape(N_HEAD, N_CTX, BLOCK_ROWS, array.shape[-1])
    picked = lax.dynamic_index_in_dim(blocks, shard, 1, keepdims=False)
    return picked.reshape(N_HEAD * BLOCK_ROWS, array.shape[-1])

def partial_terms(queries, keys, values, query_positions, key_pos):
    rows = queries.shape[0]
    kv_heads = keys.shape[1] // HEAD_DIMENSION
    group = queries.shape[1] // HEAD_DIMENSION // kv_heads
    scale = 1.0 / math.sqrt(HEAD_DIMENSION)
    qf = queries.astype(jnp.float32).reshape(rows, kv_heads, group, HEAD_DIMENSION)
    kf = keys.astype(jnp.float32).reshape(-1, kv_heads, HEAD_DIMENSION)
    vf = values.astype(jnp.float32).reshape(-1, kv_heads, HEAD_DIMENSION)
    score_matrix = jnp.einsum('rhgd,khd->hgrk', qf, kf, precision=lax.Precision.HIGHEST) * scale
    visible = key_pos[None, :] <= query_positions[:, None]
    shifted = jnp.where(visible, score_matrix, -1e+30)
    peak = jnp.maximum(lax.optimization_barrier(jnp.max(shifted, axis=-1)), -10000.0)
    weights = jnp.exp(shifted - peak[..., None])
    total = lax.optimization_barrier(jnp.sum(weights, axis=-1))
    probs = weights.astype(jnp.bfloat16).astype(jnp.float32)
    acc = jnp.einsum('hgrk,khd->rhgd', probs, vf, precision=lax.Precision.HIGHEST)
    acc = acc.reshape(rows, kv_heads * group * HEAD_DIMENSION)
    peak = peak.transpose(2, 0, 1).reshape(rows, kv_heads * group)
    total = total.transpose(2, 0, 1).reshape(rows, kv_heads * group)
    return (peak, total, acc)

def combine(first, second):
    peak_a, total_a, acc_a = first
    peak_b, total_b, acc_b = second
    peak = jnp.maximum(peak_a, peak_b)
    factor_a = jnp.exp(peak_a - peak)
    factor_b = jnp.exp(peak_b - peak)
    total = total_a * factor_a + total_b * factor_b
    rows, heads = peak.shape
    acc = acc_a.reshape(rows, heads, -1) * factor_a[..., None] + acc_b.reshape(rows, heads, -1) * factor_b[..., None]
    result = (acc / total[..., None]).reshape(rows, -1)
    return (result, peak + jnp.log(total))

def reference(query, key, value, block_order):
    rows = jnp.arange(SEQUENCE_TOKENS, dtype=jnp.int32)
    pos = block_order[rows // BLOCK_ROWS].astype(jnp.int32) * BLOCK_ROWS + rows % BLOCK_ROWS
    pos_col = pos[:, None]

    def one_shard(shard):
        before = (shard - 1) % N_CTX
        queries = shard_rows(query, shard)
        local_positions = shard_rows(pos_col, shard)[:, 0]
        prev_pos = shard_rows(pos_col, before)[:, 0]
        own = partial_terms(queries, shard_rows(key, shard), shard_rows(value, shard), local_positions, local_positions)
        far = partial_terms(queries, shard_rows(key, before), shard_rows(value, before), local_positions, prev_pos)
        result, lse = combine(own, far)
        return (result.astype(jnp.bfloat16), lse)
    results, lses = lax.map(one_shard, jnp.arange(N_CTX, dtype=jnp.int32))
    attended = results.reshape(N_CTX, N_HEAD, BLOCK_ROWS, HQ * HEAD_DIMENSION).transpose(1, 0, 2, 3).reshape(SEQUENCE_TOKENS, HQ * HEAD_DIMENSION)
    log_norm_rows = lses.reshape(N_CTX, N_HEAD, BLOCK_ROWS, HQ).transpose(1, 0, 2, 3).reshape(SEQUENCE_TOKENS, HQ)
    return (attended, log_norm_rows)
```

```python
import functools
import math

import jax
import jax.numpy as jnp
from jax import lax
from jax.experimental import pallas as pl
from jax.experimental.pallas import tpu as pltpu
from jax.sharding import PartitionSpec as P

D = 128
HIDDEN = -1e30
LOG2E = math.log2(math.e)
SCALE = LOG2E / math.sqrt(D)


def mask_bias(order, shard, head_ids, n_ctx, here_head, here_ctx, block):
    width = len(head_ids) * block
    row = lax.broadcasted_iota(jnp.int32, (block, width), 0)
    col = lax.broadcasted_iota(jnp.int32, (block, width), 1)
    query_pos = order[here_head * n_ctx + here_ctx] * block + row
    key_pos = jnp.zeros((block, width), jnp.int32)
    for j, head_id in enumerate(head_ids):
        start = order[head_id * n_ctx + shard] * block - j * block
        key_pos = jnp.where(col >= j * block, start + col, key_pos)
    return jnp.where(key_pos <= query_pos, 0.0, HIDDEN).astype(jnp.float32)


def attend(q_ref, k_refs, v_refs, bias, g, floor):
    q = q_ref[:, g * D : (g + 1) * D]
    k = jnp.concatenate([r[...] for r in k_refs], axis=0)
    v = jnp.concatenate([r[...] for r in v_refs], axis=0)
    v = jnp.concatenate([v, jnp.ones_like(v)], axis=1)
    s = lax.dot_general(q, k, (((1,), (1,)), ((), ())), preferred_element_type=jnp.float32)
    t = s * SCALE + bias
    m = jnp.max(t, axis=1, keepdims=True)
    if floor is not None:
        m = jnp.maximum(m, floor)
    p = jnp.exp2(t - m).astype(jnp.bfloat16)
    ext = jnp.dot(p, v, preferred_element_type=jnp.float32)
    return m, ext[:, :D], ext[:, D:]


def own_kernel(order, ids, q_ref, *refs, n_blocks, n_ctx, group, block):
    k_refs, v_refs = refs[:n_blocks], refs[n_blocks : 2 * n_blocks]
    out_ref, lse_ref, bias_ref = refs[2 * n_blocks :]
    here_head, here_ctx = ids[0], ids[1]

    @pl.when(pl.program_id(0) == 0)
    def _():
        bias_ref[...] = mask_bias(
            order, here_ctx, [ids[2 + j] for j in range(n_blocks)], n_ctx, here_head, here_ctx, block
        )

    lane = lax.broadcasted_iota(jnp.int32, (block, D), 1)
    lse = jnp.zeros((block, D), jnp.float32)
    for g in range(group):
        m, acc, total = attend(q_ref, k_refs, v_refs, bias_ref[...], g, None)
        out_ref[:, g * D : (g + 1) * D] = acc / total
        lse = jnp.where(lane == g, m + jnp.log2(total), lse)
    lse_ref[0] = lse


def far_kernel(order, ids, q_ref, *refs, n_blocks, n_ctx, group, block):
    k_refs, v_refs = refs[:n_blocks], refs[n_blocks : 2 * n_blocks]
    first_ref, first_lse_ref, out_ref, lse_ref, bias_ref = refs[2 * n_blocks :]
    here_head, here_ctx = ids[0], ids[1]

    @pl.when(pl.program_id(0) == 0)
    def _():
        before = jnp.where(here_ctx == 0, n_ctx - 1, here_ctx - 1)
        bias_ref[...] = mask_bias(
            order, before, [ids[2 + j] for j in range(n_blocks)], n_ctx, here_head, here_ctx, block
        )
        lse_ref[...] = jnp.zeros_like(lse_ref)

    lane = lax.broadcasted_iota(jnp.int32, (block, D), 1)
    base = pl.program_id(0) * group
    lse = lse_ref[...]
    for g in range(group):
        before_lse = first_lse_ref[0][:, g : g + 1]
        m, acc, total = attend(q_ref, k_refs, v_refs, bias_ref[...], g, before_lse)
        factor = jnp.exp2(before_lse - m)
        total = total + factor
        merged = first_ref[:, g * D : (g + 1) * D] * factor + acc
        out_ref[:, g * D : (g + 1) * D] = (merged / total).astype(out_ref.dtype)
        lse = jnp.where(lane == base + g, (m + jnp.log2(total)) / LOG2E, lse)
    lse_ref[...] = lse


def head_maps(n_blocks, kv_heads, packed):
    def at(offset):
        return lambda h, *_: (0, offset + h)

    return at(0), at(kv_heads if packed else 0)


def run(kernel, name, order, ids, query, blocks, extra, out_shape, out_specs, extra_specs):
    block, width = query.shape
    kv_heads = blocks[0][0].shape[1] // D // (2 if blocks[0][0] is blocks[0][1] else 1)
    group = width // D // kv_heads
    n_blocks = len(blocks)
    k_specs, v_specs = [], []
    for k, v in blocks:
        k_map, v_map = head_maps(n_blocks, kv_heads, k is v)
        k_specs.append(pl.BlockSpec((block, D), k_map))
        v_specs.append(pl.BlockSpec((block, D), v_map))
    return pl.pallas_call(
        functools.partial(
            kernel, n_blocks=n_blocks, n_ctx=lax.axis_size("ctx"), group=group, block=block
        ),
        out_shape=out_shape,
        grid_spec=pltpu.PrefetchScalarGridSpec(
            num_scalar_prefetch=2,
            grid=(kv_heads,),
            in_specs=[pl.BlockSpec((block, group * D), lambda h, *_: (0, h))]
            + k_specs
            + v_specs
            + extra_specs,
            out_specs=out_specs,
            scratch_shapes=[pltpu.VMEM((block, n_blocks * block), jnp.float32)],
        ),
        compiler_params=pltpu.CompilerParams(dimension_semantics=("arbitrary",)),
        cost_estimate=pl.CostEstimate(
            flops=8 * block * width * n_blocks * block, transcendentals=0, bytes_accessed=6 * block * width
        ),
        name=name,
    )(order, ids, query, *[k for k, _ in blocks], *[v for _, v in blocks], *extra)


def body(query, key, value, block_order):
    n_head = lax.axis_size("head")
    n_ctx = lax.axis_size("ctx")
    block, width = query.shape
    kv_heads = key.shape[1] // D
    group = width // D // kv_heads
    here_head = lax.axis_index("head")
    here_ctx = lax.axis_index("ctx")
    pair = 2 if n_head % 2 == 0 else 1

    def moved(array, head_step, ctx_step):
        route = []
        for h in range(n_head):
            for c in range(n_ctx):
                to = ((h + pair * head_step) % n_head) * n_ctx + (c + ctx_step) % n_ctx
                route.append((h * n_ctx + c, to))
        return lax.ppermute(array, ("head", "ctx"), route)

    def swapped(array):
        route = [(h * n_ctx + c, (h ^ 1) * n_ctx + c) for h in range(n_head) for c in range(n_ctx)]
        return lax.ppermute(array, ("head", "ctx"), route)

    mine = jnp.concatenate([key, value], axis=1)
    chips = n_head // pair
    far = [moved(mine, step, 1) for step in range(chips)]
    own = [moved(mine, step, 0) for step in range(1, chips)]
    sources = [(here_head - pair * step) % n_head for step in range(chips)]
    own_blocks = [(key, value)] + [(b, b) for b in own]
    far_blocks = [(b, b) for b in far]
    if pair == 2:
        own_blocks += [(b, b) for b in [swapped(mine)] + [swapped(b) for b in own]]
        far_blocks += [(b, b) for b in [swapped(b) for b in far]]
        sources += [s ^ 1 for s in sources]
    ids = jnp.stack([here_head, here_ctx] + sources).astype(jnp.int32)

    wide = pl.BlockSpec((block, group * D), lambda h, *_: (0, h))
    parts = pl.BlockSpec((1, block, D), lambda h, *_: (h, 0, 0))
    first, first_lse = run(
        own_kernel, "own_shard", block_order, ids, query, own_blocks, [],
        [
            jax.ShapeDtypeStruct((block, width), jnp.float32),
            jax.ShapeDtypeStruct((kv_heads, block, D), jnp.float32),
        ],
        [wide, parts], [],
    )
    return run(
        far_kernel, "far_shard", block_order, ids, query, far_blocks, [first, first_lse],
        [
            jax.ShapeDtypeStruct((block, width), jnp.bfloat16),
            jax.ShapeDtypeStruct((block, kv_heads * group), jnp.float32),
        ],
        [wide, pl.BlockSpec((block, kv_heads * group), lambda h, *_: (0, 0))], [wide, parts],
    )


def solution(mesh):
    placed = (P(("head", "ctx"), None), P(("head", "ctx"), None), P(("head", "ctx"), None), P())
    return jax.shard_map(
        body,
        mesh=mesh,
        in_specs=placed,
        out_specs=(P(("head", "ctx"), None), P(("head", "ctx"), None)),
        check_vma=False,
    )
```

```python
import functools
import math

import jax
import jax.numpy as jnp
from jax import lax
from jax.experimental import pallas as pl
from jax.experimental.pallas import tpu as pltpu
from jax.sharding import PartitionSpec as P

D = 128
HIDDEN = -1e30
HEADS = 4
CHUNK = 4
LOG2E = math.log2(math.e)
SCALE = LOG2E / math.sqrt(D)


def attend_kernel(order, q_ref, *refs, n_blocks, n_ctx, sources, group, chunk, heads, block):
    k_refs, v_refs = refs[:n_blocks], refs[n_blocks : 2 * n_blocks]
    out_ref, lse_ref, query_mark, key_mark = refs[2 * n_blocks :]

    @pl.when(pl.program_id(0) == 0)
    def _():
        row = lax.broadcasted_iota(jnp.int32, (block, D), 0)
        col = lax.broadcasted_iota(jnp.int32, (block, D), 1)
        query_mark[...] = jnp.where((col == row) | (col == block), 1.0, 0.0).astype(jnp.bfloat16)
        head, ctx = lax.axis_index("head"), lax.axis_index("ctx")
        mine = order[head * n_ctx + ctx]
        marks = [jnp.where(row > col, HIDDEN, 0.0)]
        for source in sources[1:]:
            later = order[source(head, ctx)] > mine
            marks.append(jnp.where(col == block, jnp.where(later, HIDDEN, 0.0), 0.0))
        key_mark[...] = jnp.concatenate(marks, axis=0).astype(jnp.bfloat16)
        lse_ref[...] = jnp.zeros_like(lse_ref)

    lane = lax.broadcasted_iota(jnp.int32, (block, D), 1)
    marked = jnp.concatenate([query_mark[...]] * chunk, axis=0)
    for head in range(heads):
        at = slice(head * D, (head + 1) * D)
        k = jnp.concatenate([r[:, at] for r in k_refs], axis=0)
        k = jnp.concatenate([k, key_mark[...]], axis=1)
        v = jnp.concatenate([r[:, at] for r in v_refs], axis=0)
        v = jnp.concatenate([v, jnp.ones_like(v)], axis=1)
        base = (pl.program_id(0) * heads + head) * group
        peaks = jnp.zeros((block, D), jnp.float32)
        totals = jnp.ones((block, D), jnp.float32)
        for start in range(0, group, chunk):
            first = head * group + start
            q = jnp.concatenate([q_ref[:, (first + i) * D : (first + i + 1) * D] for i in range(chunk)], axis=0)
            q = jnp.concatenate([q, marked], axis=1)
            s = lax.dot_general(q, k, (((1,), (1,)), ((), ())), preferred_element_type=jnp.float32)
            m = jnp.maximum(jnp.max(s, axis=1, keepdims=True) * SCALE, -10000.0 * LOG2E)
            p = jnp.exp2(s * SCALE - m).astype(jnp.bfloat16)
            both = jnp.dot(p, v, preferred_element_type=jnp.float32)
            acc, total = both[:, :D], both[:, D:]
            inverse = pl.reciprocal(total, approx=True)
            inverse = inverse * (2.0 - total * inverse)
            inverse = inverse * (2.0 - total * inverse)
            result = (acc * inverse).astype(out_ref.dtype)
            for i in range(chunk):
                rows = slice(i * block, (i + 1) * block)
                out_ref[:, (first + i) * D : (first + i + 1) * D] = result[rows]
                chosen = lane == base + start + i
                peaks = jnp.where(chosen, m[rows], peaks)
                totals = jnp.where(chosen, total[rows], totals)
        lse_ref[...] += (peaks + jnp.log2(totals)) * (1.0 / LOG2E)


def attend(order, query, blocks, sources, kv_heads):
    block, width = query.shape
    group = width // D // kv_heads
    heads = math.gcd(kv_heads, HEADS)
    wide = pl.BlockSpec((block, heads * group * D), lambda h, *_: (0, h))
    lse = pl.BlockSpec((block, kv_heads * group), lambda h, *_: (0, 0))
    parts = pl.BlockSpec((block, heads * D), lambda h, *_: (0, h))
    later = pl.BlockSpec((block, heads * D), lambda h, *_: (0, kv_heads // heads + h))
    n_blocks = len(blocks)
    return pl.pallas_call(
        functools.partial(
            attend_kernel, n_blocks=n_blocks, n_ctx=lax.axis_size("ctx"), sources=sources, group=group,
            chunk=math.gcd(group, CHUNK), heads=heads, block=block,
        ),
        out_shape=[
            jax.ShapeDtypeStruct((block, width), jnp.bfloat16),
            jax.ShapeDtypeStruct((block, kv_heads * group), jnp.float32),
        ],
        grid_spec=pltpu.PrefetchScalarGridSpec(
            num_scalar_prefetch=1,
            grid=(kv_heads // heads,),
            in_specs=[wide] + [parts] * n_blocks + [later if k is v else parts for k, v in blocks],
            out_specs=[wide, lse],
            scratch_shapes=[pltpu.VMEM((block, D), jnp.bfloat16), pltpu.VMEM((n_blocks * block, D), jnp.bfloat16)],
        ),
        compiler_params=pltpu.CompilerParams(dimension_semantics=("arbitrary",)),
        cost_estimate=pl.CostEstimate(
            flops=4 * block * width * n_blocks * block,
            transcendentals=block * (width // D) * n_blocks * block,
            bytes_accessed=4 * block * width,
        ),
        name="attend",
    )(order, query, *[k for k, _ in blocks], *[v for _, v in blocks])


def body(query, key, value, block_order):
    n_head = lax.axis_size("head")
    n_ctx = lax.axis_size("ctx")
    block, width = query.shape
    kv_heads = key.shape[1] // D
    pair = 2 if n_head % 2 == 0 else 1

    def moved(array, head_step, ctx_step):
        route = []
        for h in range(n_head):
            for c in range(n_ctx):
                to = ((h + pair * head_step) % n_head) * n_ctx + (c + ctx_step) % n_ctx
                route.append((h * n_ctx + c, to))
        return lax.ppermute(array, ("head", "ctx"), route)

    def swapped(array):
        route = [(h * n_ctx + c, (h ^ 1) * n_ctx + c) for h in range(n_head) for c in range(n_ctx)]
        return lax.ppermute(array, ("head", "ctx"), route)

    mine = jnp.concatenate([key, value], axis=1)
    chips = n_head // pair

    def source(head_step, ctx_step, flip):
        def at(h, c):
            h = h ^ 1 if flip else h
            return lax.rem(h - pair * head_step + n_head, n_head) * n_ctx + lax.rem(c - ctx_step + n_ctx, n_ctx)

        return at

    blocks, sources, steps = [(key, value)], [source(0, 0, False)], []
    for ctx_step in (0, 1):
        steps += [(head_step, ctx_step) for head_step in range(chips) if head_step or ctx_step]
    arrived = [moved(mine, *step) for step in steps]
    if pair == 2:
        blocks += [(b, b) for b in [swapped(mine)]]
        sources.append(source(0, 0, True))
    for step, array in zip(steps, arrived):
        blocks.append((array, array))
        sources.append(source(*step, False))
        if pair == 2:
            other = swapped(array)
            blocks.append((other, other))
            sources.append(source(*step, True))
    return attend(block_order, query, blocks, sources, kv_heads)


def solution(mesh):
    placed = (P(("head", "ctx"), None), P(("head", "ctx"), None), P(("head", "ctx"), None), P())
    return jax.shard_map(
        body,
        mesh=mesh,
        in_specs=placed,
        out_specs=(P(("head", "ctx"), None), P(("head", "ctx"), None)),
        check_vma=False,
    )
```

```python
import functools
import math

import jax
import jax.numpy as jnp
from jax import lax
from jax.experimental import pallas as pl
from jax.experimental.pallas import tpu as pltpu
from jax.sharding import PartitionSpec as P

D = 128
HIDDEN = -1e30
HEADS = 2
PIECES = 2
CHUNK = 4
LOG2E = math.log2(math.e)
SCALE = LOG2E / math.sqrt(D)


def pack(key, value, pieces):
    block, width = key.shape
    part = width // pieces

    def kernel(k_ref, v_ref, *refs):
        copies = []
        for i in range(pieces):
            for j, source in enumerate((k_ref, v_ref)):
                copies.append(
                    pltpu.make_async_copy(
                        source.at[:, i * part : (i + 1) * part],
                        refs[i].at[:, j * part : (j + 1) * part],
                        refs[pieces].at[2 * i + j],
                    )
                )
        for copy in copies:
            copy.start()
        for copy in copies:
            copy.wait()

    return pl.pallas_call(
        kernel,
        out_shape=[jax.ShapeDtypeStruct((block, 2 * part), key.dtype)] * pieces,
        in_specs=[pl.BlockSpec(memory_space=pl.ANY)] * 2,
        out_specs=[pl.BlockSpec(memory_space=pltpu.VMEM)] * pieces,
        scratch_shapes=[pltpu.SemaphoreType.DMA((2 * pieces,))],
        name="pack",
    )(key, value)


def attend_kernel(order, q_ref, *refs, n_blocks, n_ctx, sources, group, chunk, heads, block, head_start, extra):
    k_refs, v_refs = refs[:n_blocks], refs[n_blocks : 2 * n_blocks]
    out_ref, lse_ref, query_mark, key_mark = refs[2 * n_blocks + extra :]

    @pl.when(pl.program_id(0) == 0)
    def _():
        row = lax.broadcasted_iota(jnp.int32, (block, D), 0)
        col = lax.broadcasted_iota(jnp.int32, (block, D), 1)
        query_mark[...] = jnp.where((col == row) | (col == block), 1.0, 0.0).astype(jnp.bfloat16)
        head, ctx = lax.axis_index("head"), lax.axis_index("ctx")
        mine = order[head * n_ctx + ctx]
        marks = [jnp.where(row > col, HIDDEN, 0.0)]
        for source in sources[1:]:
            later = order[source(head, ctx)] > mine
            marks.append(jnp.where(col == block, jnp.where(later, HIDDEN, 0.0), 0.0))
        key_mark[...] = jnp.concatenate(marks, axis=0).astype(jnp.bfloat16)
        lse_ref[...] = refs[2 * n_blocks][...] if extra else jnp.zeros_like(lse_ref)

    lane = lax.broadcasted_iota(jnp.int32, (block, D), 1)
    marked = jnp.concatenate([query_mark[...]] * chunk, axis=0)
    for head in range(heads):
        at = slice(head * D, (head + 1) * D)
        k = jnp.concatenate([r[:, at] for r in k_refs], axis=0)
        k = jnp.concatenate([k, key_mark[...]], axis=1)
        v = jnp.concatenate([r[:, at] for r in v_refs], axis=0)
        v = jnp.concatenate([v, jnp.ones_like(v)], axis=1)
        base = (head_start + pl.program_id(0) * heads + head) * group
        peaks = jnp.zeros((block, D), jnp.float32)
        totals = jnp.ones((block, D), jnp.float32)
        for start in range(0, group, chunk):
            first = head * group + start
            q = jnp.concatenate([q_ref[:, (first + i) * D : (first + i + 1) * D] for i in range(chunk)], axis=0)
            q = jnp.concatenate([q, marked], axis=1)
            s = lax.dot_general(q, k, (((1,), (1,)), ((), ())), preferred_element_type=jnp.float32)
            m = jnp.maximum(jnp.max(s, axis=1, keepdims=True) * SCALE, -10000.0 * LOG2E)
            p = jnp.exp2(s * SCALE - m).astype(jnp.bfloat16)
            both = jnp.dot(p, v, preferred_element_type=jnp.float32)
            acc, total = both[:, :D], both[:, D:]
            inverse = pl.reciprocal(total, approx=True)
            inverse = inverse * (2.0 - total * inverse)
            inverse = inverse * (2.0 - total * inverse)
            result = (acc * inverse).astype(out_ref.dtype)
            for i in range(chunk):
                rows = slice(i * block, (i + 1) * block)
                out_ref[:, (first + i) * D : (first + i + 1) * D] = result[rows]
                chosen = lane == base + start + i
                peaks = jnp.where(chosen, m[rows], peaks)
                totals = jnp.where(chosen, total[rows], totals)
        lse_ref[...] += (peaks + jnp.log2(totals)) * (1.0 / LOG2E)


def attend(order, query, blocks, sources, kv_heads, head_start, head_count, before):
    block, width = query.shape
    group = width // D // kv_heads
    heads = math.gcd(head_count, HEADS)
    steps, skip = head_count // heads, head_start // heads
    wide = pl.BlockSpec((block, heads * group * D), lambda h, *_: (0, skip + h))
    lse = pl.BlockSpec((block, kv_heads * group), lambda h, *_: (0, 0))
    whole = pl.BlockSpec((block, heads * D), lambda h, *_: (0, skip + h))
    parts = pl.BlockSpec((block, heads * D), lambda h, *_: (0, h))
    later = pl.BlockSpec((block, heads * D), lambda h, *_: (0, steps + h))
    n_blocks = len(blocks)
    extra = () if before is None else (before[1], before[0])
    return pl.pallas_call(
        functools.partial(
            attend_kernel, n_blocks=n_blocks, n_ctx=lax.axis_size("ctx"), sources=sources, group=group,
            chunk=math.gcd(group, CHUNK), heads=heads, block=block, head_start=head_start, extra=len(extra),
        ),
        out_shape=[
            jax.ShapeDtypeStruct((block, width), jnp.bfloat16),
            jax.ShapeDtypeStruct((block, kv_heads * group), jnp.float32),
        ],
        grid_spec=pltpu.PrefetchScalarGridSpec(
            num_scalar_prefetch=1,
            grid=(steps,),
            in_specs=[wide]
            + [parts if k is v else whole for k, v in blocks]
            + [later if k is v else whole for k, v in blocks]
            + ([lse, pl.BlockSpec(memory_space=pl.ANY)] if extra else []),
            out_specs=[wide, lse],
            scratch_shapes=[pltpu.VMEM((block, D), jnp.bfloat16), pltpu.VMEM((n_blocks * block, D), jnp.bfloat16)],
        ),
        input_output_aliases={2 + 2 * n_blocks + 1: 0} if extra else {},
        compiler_params=pltpu.CompilerParams(dimension_semantics=("arbitrary",)),
        cost_estimate=pl.CostEstimate(
            flops=4 * block * width * n_blocks * block * head_count // kv_heads,
            transcendentals=block * (width // D) * n_blocks * block * head_count // kv_heads,
            bytes_accessed=4 * block * width * head_count // kv_heads,
        ),
        name="attend",
    )(order, query, *[k for k, _ in blocks], *[v for _, v in blocks], *extra)


def body(query, key, value, block_order):
    n_head = lax.axis_size("head")
    n_ctx = lax.axis_size("ctx")
    block, width = query.shape
    kv_heads = key.shape[1] // D
    pair = 2 if n_head % 2 == 0 else 1

    def moved(array, head_step, ctx_step):
        route = []
        for h in range(n_head):
            for c in range(n_ctx):
                to = ((h + pair * head_step) % n_head) * n_ctx + (c + ctx_step) % n_ctx
                route.append((h * n_ctx + c, to))
        return lax.ppermute(array, ("head", "ctx"), route)

    def swapped(array):
        route = [(h * n_ctx + c, (h ^ 1) * n_ctx + c) for h in range(n_head) for c in range(n_ctx)]
        return lax.ppermute(array, ("head", "ctx"), route)

    pieces = math.gcd(kv_heads, PIECES)
    chips = n_head // pair

    def source(head_step, ctx_step, flip):
        def at(h, c):
            h = h ^ 1 if flip else h
            return lax.rem(h - pair * head_step + n_head, n_head) * n_ctx + lax.rem(c - ctx_step + n_ctx, n_ctx)

        return at

    steps = [(step, ctx_step) for ctx_step in (0, 1) for step in range(chips) if step or ctx_step]
    count = kv_heads // pieces
    packed = pack(key, value, pieces)
    arrived = [[moved(mine, *step) for step in steps] for mine in packed]
    done = None
    for piece in range(pieces):
        blocks, sources = [(key, value)], [source(0, 0, False)]
        if pair == 2:
            other = swapped(packed[piece])
            blocks.append((other, other))
            sources.append(source(0, 0, True))
        for step, array in zip(steps, arrived[piece]):
            blocks.append((array, array))
            sources.append(source(*step, False))
            if pair == 2:
                other = swapped(array)
                blocks.append((other, other))
                sources.append(source(*step, True))
        done = attend(block_order, query, blocks, sources, kv_heads, piece * count, count, done)
    return done


def solution(mesh):
    placed = (P(("head", "ctx"), None), P(("head", "ctx"), None), P(("head", "ctx"), None), P())
    return jax.shard_map(
        body,
        mesh=mesh,
        in_specs=placed,
        out_specs=(P(("head", "ctx"), None), P(("head", "ctx"), None)),
        check_vma=False,
    )
```

```python
import functools
import math

import jax
import jax.numpy as jnp
from jax import lax
from jax.experimental import pallas as pl
from jax.experimental.pallas import tpu as pltpu
from jax.sharding import PartitionSpec as P

D = 128
HIDDEN = -1e30
HEADS = 4
PIECES = 2
CHUNK = 4
LOG2E = math.log2(math.e)
SCALE = LOG2E / math.sqrt(D)


def pack(key, value, pieces):
    block, width = key.shape
    part = width // pieces

    def kernel(k_ref, v_ref, *refs):
        copies = []
        for i in range(pieces):
            for j, source in enumerate((k_ref, v_ref)):
                copies.append(
                    pltpu.make_async_copy(
                        source.at[:, i * part : (i + 1) * part],
                        refs[i].at[:, j * part : (j + 1) * part],
                        refs[pieces].at[2 * i + j],
                    )
                )
        for copy in copies:
            copy.start()
        for copy in copies:
            copy.wait()

    return pl.pallas_call(
        kernel,
        out_shape=[jax.ShapeDtypeStruct((block, 2 * part), key.dtype)] * pieces,
        in_specs=[pl.BlockSpec(memory_space=pl.ANY)] * 2,
        out_specs=[pl.BlockSpec(memory_space=pltpu.VMEM)] * pieces,
        scratch_shapes=[pltpu.SemaphoreType.DMA((2 * pieces,))],
        name="pack",
    )(key, value)


def attend_kernel(order, q_ref, *refs, n_blocks, n_ctx, sources, group, chunk, heads, block, head_start, extra):
    k_refs, v_refs = refs[:n_blocks], refs[n_blocks : 2 * n_blocks]
    out_ref, lse_ref, query_mark, key_mark = refs[2 * n_blocks + extra :]

    @pl.when(pl.program_id(0) == 0)
    def _():
        row = lax.broadcasted_iota(jnp.int32, (block, D), 0)
        col = lax.broadcasted_iota(jnp.int32, (block, D), 1)
        query_mark[...] = jnp.where((col == row) | (col == block), 1.0, 0.0).astype(jnp.bfloat16)
        head, ctx = lax.axis_index("head"), lax.axis_index("ctx")
        mine = order[head * n_ctx + ctx]
        marks = [jnp.where(row > col, HIDDEN, 0.0)]
        for source in sources[1:]:
            later = order[source(head, ctx)] > mine
            marks.append(jnp.where(col == block, jnp.where(later, HIDDEN, 0.0), 0.0))
        key_mark[...] = jnp.concatenate(marks, axis=0).astype(jnp.bfloat16)
        lse_ref[...] = refs[2 * n_blocks][...] if extra else jnp.zeros_like(lse_ref)

    lane = lax.broadcasted_iota(jnp.int32, (block, D), 1)
    marked = jnp.concatenate([query_mark[...]] * chunk, axis=0)
    for head in range(heads):
        at = slice(head * D, (head + 1) * D)
        k = jnp.concatenate([r[:, at] for r in k_refs], axis=0)
        k = jnp.concatenate([k, key_mark[...]], axis=1)
        v = jnp.concatenate([r[:, at] for r in v_refs], axis=0)
        v = jnp.concatenate([v, jnp.ones_like(v)], axis=1)
        base = (head_start + pl.program_id(0) * heads + head) * group
        peaks = jnp.zeros((block, D), jnp.float32)
        totals = jnp.ones((block, D), jnp.float32)
        for start in range(0, group, chunk):
            first = head * group + start
            q = jnp.concatenate([q_ref[:, (first + i) * D : (first + i + 1) * D] for i in range(chunk)], axis=0)
            q = jnp.concatenate([q, marked], axis=1)
            s = lax.dot_general(q, k, (((1,), (1,)), ((), ())), preferred_element_type=jnp.float32)
            m = jnp.maximum(jnp.max(s, axis=1, keepdims=True) * SCALE, -10000.0 * LOG2E)
            p = jnp.exp2(s * SCALE - m).astype(jnp.bfloat16)
            both = jnp.dot(p, v, preferred_element_type=jnp.float32)
            acc, total = both[:, :D], both[:, D:]
            inverse = pl.reciprocal(total, approx=True)
            inverse = inverse * (2.0 - total * inverse)
            inverse = inverse * (2.0 - total * inverse)
            result = (acc * inverse).astype(out_ref.dtype)
            for i in range(chunk):
                rows = slice(i * block, (i + 1) * block)
                out_ref[:, (first + i) * D : (first + i + 1) * D] = result[rows]
                chosen = lane == base + start + i
                peaks = jnp.where(chosen, m[rows], peaks)
                totals = jnp.where(chosen, total[rows], totals)
        lse_ref[...] += (peaks + jnp.log2(totals)) * (1.0 / LOG2E)


def attend(order, query, blocks, sources, kv_heads, head_start, head_count, before):
    block, width = query.shape
    group = width // D // kv_heads
    heads = math.gcd(head_count, HEADS)
    steps, skip = head_count // heads, head_start // heads
    wide = pl.BlockSpec((block, heads * group * D), lambda h, *_: (0, skip + h))
    lse = pl.BlockSpec((block, kv_heads * group), lambda h, *_: (0, 0))
    whole = pl.BlockSpec((block, heads * D), lambda h, *_: (0, skip + h))
    parts = pl.BlockSpec((block, heads * D), lambda h, *_: (0, h))
    later = pl.BlockSpec((block, heads * D), lambda h, *_: (0, steps + h))
    n_blocks = len(blocks)
    extra = () if before is None else (before[1], before[0])
    return pl.pallas_call(
        functools.partial(
            attend_kernel, n_blocks=n_blocks, n_ctx=lax.axis_size("ctx"), sources=sources, group=group,
            chunk=math.gcd(group, CHUNK), heads=heads, block=block, head_start=head_start, extra=len(extra),
        ),
        out_shape=[
            jax.ShapeDtypeStruct((block, width), jnp.bfloat16),
            jax.ShapeDtypeStruct((block, kv_heads * group), jnp.float32),
        ],
        grid_spec=pltpu.PrefetchScalarGridSpec(
            num_scalar_prefetch=1,
            grid=(steps,),
            in_specs=[wide]
            + [parts if k is v else whole for k, v in blocks]
            + [later if k is v else whole for k, v in blocks]
            + ([lse, pl.BlockSpec(memory_space=pl.ANY)] if extra else []),
            out_specs=[wide, lse],
            scratch_shapes=[pltpu.VMEM((block, D), jnp.bfloat16), pltpu.VMEM((n_blocks * block, D), jnp.bfloat16)],
        ),
        input_output_aliases={2 + 2 * n_blocks + 1: 0} if extra else {},
        compiler_params=pltpu.CompilerParams(dimension_semantics=("arbitrary",)),
        cost_estimate=pl.CostEstimate(
            flops=4 * block * width * n_blocks * block * head_count // kv_heads,
            transcendentals=block * (width // D) * n_blocks * block * head_count // kv_heads,
            bytes_accessed=4 * block * width * head_count // kv_heads,
        ),
        name="attend",
    )(order, query, *[k for k, _ in blocks], *[v for _, v in blocks], *extra)


def body(query, key, value, block_order):
    n_head = lax.axis_size("head")
    n_ctx = lax.axis_size("ctx")
    block, width = query.shape
    kv_heads = key.shape[1] // D
    pair = 2 if n_head % 2 == 0 else 1

    def moved(array, head_step, ctx_step):
        route = []
        for h in range(n_head):
            for c in range(n_ctx):
                to = ((h + pair * head_step) % n_head) * n_ctx + (c + ctx_step) % n_ctx
                route.append((h * n_ctx + c, to))
        return lax.ppermute(array, ("head", "ctx"), route)

    def swapped(array):
        route = [(h * n_ctx + c, (h ^ 1) * n_ctx + c) for h in range(n_head) for c in range(n_ctx)]
        return lax.ppermute(array, ("head", "ctx"), route)

    pieces = math.gcd(kv_heads, PIECES)
    chips = n_head // pair

    def source(head_step, ctx_step, flip):
        def at(h, c):
            h = h ^ 1 if flip else h
            return lax.rem(h - pair * head_step + n_head, n_head) * n_ctx + lax.rem(c - ctx_step + n_ctx, n_ctx)

        return at

    steps = [(step, ctx_step) for ctx_step in (0, 1) for step in range(chips) if step or ctx_step]
    count = kv_heads // pieces
    packed = pack(key, value, pieces)
    arrived = [[moved(mine, *step) for step in steps] for mine in packed]
    done = None
    for piece in range(pieces):
        blocks, sources = [(key, value)], [source(0, 0, False)]
        if pair == 2:
            other = swapped(packed[piece])
            blocks.append((other, other))
            sources.append(source(0, 0, True))
        landed = arrived[piece]
        if done is not None:
            *landed, _ = lax.optimization_barrier((*landed, done[1]))
        for step, array in zip(steps, landed):
            blocks.append((array, array))
            sources.append(source(*step, False))
            if pair == 2:
                other = swapped(array)
                blocks.append((other, other))
                sources.append(source(*step, True))
        done = attend(block_order, query, blocks, sources, kv_heads, piece * count, count, done)
    return done


def solution(mesh):
    placed = (P(("head", "ctx"), None), P(("head", "ctx"), None), P(("head", "ctx"), None), P())
    return jax.shard_map(
        body,
        mesh=mesh,
        in_specs=placed,
        out_specs=(P(("head", "ctx"), None), P(("head", "ctx"), None)),
        check_vma=False,
    )
```
